32 devices in a mesh: rep: 2 (over x), seq: 16 (over z, y, core).
Axes of the slice: x: 2, y: 2, z: 4, core: 2. Of those that a mesh axis runs over, the one named last changes fastest.
Arguments:
- queries: bfloat16 [32, 8192], P('rep', 'seq'), parts along dimension 0, may hold values from -8 to 8
- key_pages: bfloat16 [256, 128, 1024], P(('rep', 'seq')), parts along dimension 0, may hold values from -6 to 6
- value_pages: bfloat16 [256, 128, 1024], P(('rep', 'seq')), parts along dimension 0, may hold values from -6 to 6
- page_table: int32 [32, 8], P('rep'), parts along dimension 0, may hold values from -1 to 127, as said below
- lengths: int32 [32], P('rep'), parts along dimension 0, may hold values from 1 to 1024, as said below
Outputs:
- attention_out: bfloat16 [32, 8192], P('rep', 'seq'), parts along dimension 0
- log_norm: float32 [32, 64], P('rep'), parts along dimension 0
The draws below stay inside these ranges and needn't reach their ends.
There are 2 independent parts, one for each index of `rep`. The reference program is written for one: setup_inputs(seed, part) draws one part's arguments, and reference() takes and returns one part's arrays. A program takes and returns all parts, laid end to end along the dimension named above; each array names one. Nothing has to cross between parts.
Inputs may be any that keep to these rules, and one draw needn't show every extreme that they name: `page_table`: entry j of request r is a global slot id (device index along seq times 8 plus the slot on that device) for j < ceil(lengths[r] / 128) and -1 after; no slot id appears twice; exactly 32 slots are in use in all; the slots in use on each device are its first ones, at least one; some device uses all 8; some request uses 8 pages. `lengths`: A request with 8 pages has 1024 tokens.
All inputs are finite; a program needn't handle non-finite values.
Results may differ from the reference program's by a relative error of at most 0.0085.
Values may be sent and summed in bfloat16 or wider, within the bound.
A program may use at most 64 MiB of HBM per device.

```python
import math
import jax
import jax.numpy as jnp
from jax import lax

QH = 64
KVH = 8
HEAD = 128
PAGE = 128
REQUESTS = 16
P_DEV = 8
SLOTS = 128
TOTALP = 32
MAXP = 8


def fill_numbers(key, item_count, most_each, sum_total, tier_levels):
    key_tier, key_force, key_noise = jax.random.split(key, 3)
    optional = item_count * (most_each - 1)
    owners = jnp.arange(optional, dtype=jnp.int32) // (most_each - 1)
    tier_bias = jax.random.randint(key_tier, (item_count,), 0, tier_levels) * 2048
    forced = jax.random.randint(key_force, (), 0, item_count)
    noise_bits = jax.random.randint(key_noise, (optional,), 0, 4096)
    scores = jnp.where(owners == forced, -1, noise_bits + tier_bias[owners])
    scores = scores * optional + jnp.arange(optional, dtype=jnp.int32)
    ordering = jnp.argsort(scores, stable=True)
    chosen = jnp.zeros((optional,), jnp.int32).at[ordering[:sum_total - item_count]].set(1)
    return 1 + jax.ops.segment_sum(chosen, owners, num_segments=item_count)


def paging(key):
    devices = SLOTS // P_DEV
    load_counts = fill_numbers(jax.random.fold_in(key, 101), devices, P_DEV, TOTALP, 4)
    page_counts = fill_numbers(jax.random.fold_in(key, 102), REQUESTS, MAXP, TOTALP, 2)
    slot_ids = jnp.arange(SLOTS, dtype=jnp.int32)
    is_live = slot_ids % P_DEV < load_counts[slot_ids // P_DEV]
    noise_bits = jax.random.randint(jax.random.fold_in(key, 103), (SLOTS,), 0, 4096)
    scores = (jnp.where(is_live, 0, 4096) + noise_bits) * SLOTS + slot_ids
    ordering = jnp.argsort(scores, stable=True).astype(jnp.int32)
    starts = jnp.cumsum(page_counts) - page_counts
    columns = jnp.arange(MAXP, dtype=jnp.int32)
    positions = jnp.minimum(starts[:, None] + columns[None, :], SLOTS - 1)
    page_table = jnp.where(columns[None, :] < page_counts[:, None], ordering[positions], -1)
    tail_rows = jax.random.randint(jax.random.fold_in(key, 104), (REQUESTS,), 1, PAGE + 1)
    tail_rows = jnp.where(page_counts == MAXP, PAGE, tail_rows)
    lengths = (page_counts - 1) * PAGE + tail_rows
    return (page_table.astype(jnp.int32), lengths.astype(jnp.int32))


def draw_page_table(key, part):
    return paging(key)[0]


def draw_lengths(key, part):
    return paging(key)[1]


def draw_key_pages(key, part):
    samples = jnp.clip(jax.random.normal(jax.random.fold_in(key, 203), (SLOTS, PAGE, KVH * HEAD), jnp.float32), -6.0, 6.0)
    return samples.astype(jnp.bfloat16)


def draw_queries(key, part):
    samples = jnp.clip(2.0 * jax.random.normal(jax.random.fold_in(key, 303), (REQUESTS, QH, HEAD), jnp.float32), -8.0, 8.0)
    return samples.reshape(REQUESTS, QH * HEAD).astype(jnp.bfloat16)


def steps_of(own_key, extent, pieces, smallest, high):
    gain = 1.0
    for axis_at, parts in pieces:
        draws = jax.random.uniform(jax.random.fold_in(jax.random.fold_in(own_key, 6), axis_at), (parts,), jnp.float32, smallest / len(pieces), high / len(pieces))
        gain = gain * jnp.repeat(jnp.exp(draws), extent[axis_at] // parts).reshape((-1,) + (1,) * (len(extent) - 1 - axis_at))
    return gain


def bell_draw(own_key, dims, spread, limit, pieces=(), kind=jnp.bfloat16):
    drawn = spread * jax.random.normal(own_key, dims, jnp.float32)
    if pieces:
        drawn = drawn * steps_of(own_key, dims, pieces, -0.22, 0.18)
    return jnp.clip(drawn, -limit, limit).astype(kind)


def setup_inputs(seed: int = 0, part: int = 0) -> dict:
    streams_of = jax.random.split(jax.random.key(seed), 6)
    part_splits = jax.random.split(jax.random.fold_in(streams_of[5], part), 6)
    queries = draw_queries(jax.random.fold_in(jax.random.fold_in(streams_of[5], part), 71), part)
    key_pages = draw_key_pages(jax.random.fold_in(jax.random.fold_in(streams_of[5], part), 71), part)
    value_pages = bell_draw(part_splits[2], (SLOTS, PAGE, KVH * HEAD), 1.0, 6.0, ((0, 16),))
    page_table = draw_page_table(jax.random.fold_in(jax.random.fold_in(streams_of[5], part), 71), part)
    lengths = draw_lengths(jax.random.fold_in(jax.random.fold_in(streams_of[5], part), 71), part)
    return {"queries": queries, "key_pages": key_pages, "value_pages": value_pages, "page_table": page_table, "lengths": lengths}


def reference(queries, key_pages, value_pages, page_table, lengths):
    group_size = QH // KVH

    def attend(operands):
        query_row, table_row, length_row = operands
        slot_ids = jnp.maximum(table_row, 0).astype(jnp.int32)
        keys_all = key_pages[slot_ids].reshape(MAXP * PAGE, KVH, HEAD).astype(jnp.float32)
        values_all = value_pages[slot_ids].reshape(MAXP * PAGE, KVH, HEAD).astype(jnp.float32)
        head_rows = query_row.reshape(KVH, group_size, HEAD).astype(jnp.float32)
        scores = jnp.einsum('kgd,tkd->kgt', head_rows, keys_all) / math.sqrt(HEAD)
        is_valid = jnp.arange(MAXP * PAGE, dtype=jnp.int32) < length_row
        scores = jnp.where(is_valid[None, None, :], scores, -jnp.inf)
        row_peak = lax.optimization_barrier(jnp.max(scores, axis=-1))
        weights = jnp.exp(scores - row_peak[:, :, None])
        denominator = lax.optimization_barrier(jnp.sum(weights, axis=-1))
        rounded = lax.optimization_barrier(weights.astype(jnp.bfloat16)).astype(jnp.float32)
        numerator = jnp.einsum('kgt,tkd->kgd', rounded, values_all)
        result = (numerator / denominator[:, :, None]).reshape(QH * HEAD).astype(jnp.bfloat16)
        norms = (row_peak + jnp.log(denominator)).reshape(QH)
        return (result, norms)
    outputs, norm_rows = lax.map(attend, (queries, page_table, lengths))
    return (outputs, norm_rows)
```

```python
import functools
import math

import jax
import jax.numpy as jnp
from jax import lax
from jax.experimental import pallas as pl
from jax.experimental.pallas import tpu as pltpu
from jax.sharding import PartitionSpec as P

QH = 64
KVH = 8
HEAD = 128


floor_value = -1000000000.0


def attend_block(block_index, running, pool_keys, pool_values, pool_req, pool_tok, whole_queries):
    run_max, run_sum, run_out = running
    per_step = 4
    requests = whole_queries.shape[0]
    page_rows = pool_keys.shape[1]
    group_size = QH // KVH
    start_slot = block_index * per_step
    block_keys = lax.dynamic_slice_in_dim(pool_keys, start_slot, per_step, 0).reshape(
        per_step, page_rows, KVH, HEAD
    )
    block_values = lax.dynamic_slice_in_dim(pool_values, start_slot, per_step, 0).reshape(
        per_step, page_rows, KVH, HEAD
    )
    block_req = lax.dynamic_slice_in_dim(pool_req, start_slot, per_step, 0)
    block_tok = lax.dynamic_slice_in_dim(pool_tok, start_slot, per_step, 0)
    block_queries = whole_queries[block_req].reshape(per_step, KVH, group_size, HEAD)
    scores = jnp.einsum(
        "bkgd,btkd->bkgt", block_queries, block_keys, preferred_element_type=jnp.float32
    ) * (1.0 / math.sqrt(HEAD))
    is_valid = jnp.arange(page_rows, dtype=jnp.int32)[None, :] < block_tok[:, None]
    scores = jnp.where(is_valid[:, None, None, :], scores, floor_value)
    page_max = jnp.max(scores, axis=-1)
    weights = jnp.where(is_valid[:, None, None, :], jnp.exp(scores - page_max[..., None]), 0.0)
    page_sum = jnp.sum(weights, axis=-1).reshape(per_step, QH)
    page_out = jnp.einsum(
        "bkgt,btkd->bkgd",
        weights.astype(jnp.bfloat16),
        block_values,
        preferred_element_type=jnp.float32,
    ).reshape(per_step, QH, HEAD)
    page_max = page_max.reshape(per_step, QH)
    belongs = (block_req[:, None] == jnp.arange(requests, dtype=jnp.int32)[None, :]) & (
        block_tok[:, None] > 0
    )
    candidate = jnp.where(belongs[:, :, None], page_max[:, None, :], floor_value)
    new_max = jnp.maximum(run_max, jnp.max(candidate, axis=0))
    keep_scale = jnp.where(run_max > 0.5 * floor_value, jnp.exp(run_max - new_max), 0.0)
    mixing = jnp.where(belongs[:, :, None], jnp.exp(candidate - new_max[None, :, :]), 0.0)
    run_sum = run_sum * keep_scale + jnp.sum(mixing * page_sum[:, None, :], axis=0)
    run_out = run_out * keep_scale[:, :, None] + jnp.einsum(
        "brh,bhd->rhd", mixing, page_out, precision=lax.Precision.HIGHEST
    )
    return (run_max * 0.0 + new_max, run_sum, run_out)


def generic_body(queries, key_pages, value_pages, page_table, lengths):
    slot_count = key_pages.shape[0]
    page_rows = key_pages.shape[1]
    requests, max_pages = page_table.shape
    devices = lax.axis_size("seq")
    my_index = lax.axis_index("seq")
    whole_queries = lax.all_gather(queries, "seq", axis=1, tiled=True)
    entry_ids = page_table.reshape(-1)
    entry_req = jnp.repeat(jnp.arange(requests, dtype=jnp.int32), max_pages)
    entry_tok = jnp.clip(
        lengths[:, None] - jnp.arange(max_pages, dtype=jnp.int32)[None, :] * page_rows, 0, page_rows
    ).reshape(-1)
    entry_dev = jnp.where(entry_ids >= 0, entry_ids // slot_count, -1)
    local_ids = entry_ids - my_index * slot_count
    slot_range = jnp.arange(slot_count, dtype=jnp.int32)
    matches = (entry_dev[None, :] == my_index) & (local_ids[None, :] == slot_range[:, None])
    pool_req = jnp.sum(jnp.where(matches, entry_req[None, :], 0), axis=1)
    pool_tok = jnp.sum(jnp.where(matches, entry_tok[None, :], 0), axis=1)
    per_step = 4
    block_total = slot_count // per_step
    start_state = (
        jnp.full((requests, QH), floor_value, jnp.float32),
        jnp.zeros((requests, QH), jnp.float32),
        jnp.zeros((requests, QH, HEAD), jnp.float32),
    )

    def step_block(block_index, running):
        return attend_block(
            block_index, running, key_pages, value_pages, pool_req, pool_tok, whole_queries
        )

    run_max, run_sum, run_out = lax.fori_loop(0, block_total, step_block, start_state)
    width_dev = QH * HEAD // devices
    col_heads = (my_index * width_dev + jnp.arange(width_dev, dtype=jnp.int32)) // HEAD
    pieces = lax.all_to_all(
        run_out.reshape(requests, QH * HEAD).astype(jnp.bfloat16),
        "seq",
        split_axis=1,
        concat_axis=0,
        tiled=True,
    ).astype(jnp.float32)
    every_max, every_sum = (
        lax.all_gather(run_max[None], "seq", axis=0, tiled=True),
        lax.all_gather(run_sum[None], "seq", axis=0, tiled=True),
    )
    top_max = jnp.max(every_max, axis=0)
    factor = jnp.exp(every_max - top_max[None])
    totals = jnp.sum(every_sum * factor, axis=0)
    col_factor = jnp.take(factor, col_heads, axis=2)
    shares = jnp.sum(pieces.reshape(devices, requests, width_dev) * col_factor, axis=0)
    denominators = jnp.take(totals, col_heads, axis=1)
    attention_out = (shares / denominators).astype(jnp.bfloat16)
    log_norm = top_max + jnp.log(totals)
    return (attention_out, log_norm)


def dot_f32(a, b, contract):
    return lax.dot_general(
        a, b, (contract, ((), ())), precision=lax.Precision.HIGHEST, preferred_element_type=jnp.float32
    )


def kernel(
    n,
    q_ref,
    k_hbm,
    v_hbm,
    pt_ref,
    len_ref,
    out_ref,
    norm_ref,
    k_vm,
    v_vm,
    q_stage,
    q_recv,
    q_rows,
    o_rows,
    o_stage,
    o_recv,
    st_stage,
    st_recv,
    e_rows,
    k_sem,
    v_sem,
    qs_sem,
    qr_sem,
    os_sem,
    or_sem,
    ss_sem,
    sr_sem,
):
    me = lax.axis_index("seq")
    slots, page_rows = k_vm.shape[:2]
    requests, max_pages = pt_ref.shape
    total_slots = n * slots
    heads_dev = q_ref.shape[1] // HEAD
    group = QH // KVH

    k_copies = [pltpu.make_async_copy(k_hbm.at[s], k_vm.at[s], k_sem.at[s]) for s in range(slots)]
    v_copies = [pltpu.make_async_copy(v_hbm.at[s], v_vm.at[s], v_sem.at[s]) for s in range(slots)]
    for copy in k_copies + v_copies:
        copy.start()

    barrier = pltpu.get_barrier_semaphore()
    for i in range(1, n):
        pl.semaphore_signal(
            barrier, inc=1, device_id={"seq": lax.rem(me + i, n)}, device_id_type=pl.DeviceIdType.MESH
        )

    table = pt_ref[...]
    row_at = lax.broadcasted_iota(jnp.int32, (requests, 1), 0)
    len_col = jnp.zeros((requests, 1), jnp.int32)
    for r in range(requests):
        len_col = jnp.where(row_at == r, len_ref[r], len_col)
    slot_lane = lax.broadcasted_iota(jnp.int32, (requests, total_slots), 1)
    local_lane = lax.broadcasted_iota(jnp.int32, (requests, 128), 1)
    belongs = jnp.zeros((requests, total_slots), jnp.float32)
    local_tok = jnp.zeros((requests, 128), jnp.int32)
    for j in range(max_pages):
        entry = table[:, j : j + 1]
        belongs = jnp.where(slot_lane == entry, 1.0, belongs)
        tok = jnp.clip(len_col - j * page_rows, 0, page_rows)
        local_tok = jnp.where(local_lane + me * slots == entry, tok, local_tok)
    local_tok = jnp.max(local_tok, axis=0, keepdims=True)

    belongs_t = jnp.transpose(belongs)
    picked = jnp.dot(
        belongs_t.astype(jnp.bfloat16), q_ref[...], preferred_element_type=jnp.float32
    )
    picked = jnp.concatenate(
        [
            picked[:, h * HEAD : (h + 1) * HEAD].reshape(n, slots, HEAD)
            for h in range(heads_dev)
        ],
        axis=1,
    )
    q_stage[...] = picked.astype(jnp.bfloat16)
    req_col = lax.broadcasted_iota(jnp.int32, (requests, 128), 0).astype(jnp.bfloat16) + 1
    slot_req = jnp.dot(
        belongs_t.astype(jnp.bfloat16), req_col, preferred_element_type=jnp.float32
    )

    pl.semaphore_wait(barrier, n - 1)

    def exchange(stage_of, recv, send_sem, recv_sem):
        copies = []
        for i in range(1, n):
            dst = lax.rem(me + i, n)
            copies.append(
                pltpu.make_async_remote_copy(
                    src_ref=stage_of(dst),
                    dst_ref=recv.at[me],
                    send_sem=send_sem.at[i],
                    recv_sem=recv_sem.at[i],
                    device_id={"seq": dst},
                    device_id_type=pl.DeviceIdType.MESH,
                )
            )
            copies[-1].start()
        return copies

    q_copies = exchange(lambda dst: q_stage.at[dst], q_recv, qs_sem, qr_sem)
    q_recv[me] = q_stage[me]
    for copy in q_copies:
        copy.wait_recv()
    q_rows[...] = q_recv[...].astype(jnp.float32).reshape(QH * slots, HEAD)

    scale = 1.0 / math.sqrt(HEAD)
    tok_lane = lax.broadcasted_iota(jnp.int32, (group, page_rows), 1)
    stat_lane = lax.broadcasted_iota(jnp.int32, (group, 128), 1)
    tops = [jnp.zeros((group, 128), jnp.float32) for _ in range(KVH)]
    sums = [jnp.ones((group, 128), jnp.float32) for _ in range(KVH)]
    weights = {}
    for s in range(slots):
        k_copies[s].wait()
        is_valid = tok_lane < local_tok[:, s : s + 1]
        for k in range(KVH):
            q = q_rows[pl.ds(k * group * slots + s, group, stride=slots), :].astype(jnp.bfloat16)
            scores = lax.dot_general(
                q,
                k_vm[s, :, k * HEAD : (k + 1) * HEAD],
                (((1,), (1,)), ((), ())),
                preferred_element_type=jnp.float32,
            )
            scores = jnp.where(is_valid, scores * scale, floor_value)
            top = jnp.max(scores, axis=1, keepdims=True)
            expo = jnp.exp(scores - top)
            total = jnp.sum(expo, axis=1, keepdims=True)
            tops[k] = jnp.where(stat_lane == s, top, tops[k])
            sums[k] = jnp.where(stat_lane == s, total, sums[k])
            weights[s, k] = (expo.astype(jnp.bfloat16), total)
    lse = jnp.concatenate(tops, axis=0) + jnp.log(jnp.concatenate(sums, axis=0))
    lse = jnp.concatenate([lse, jnp.zeros((128 - QH, 128), jnp.float32)], axis=0)
    st_stage[...] = jnp.transpose(lse)[:slots]
    st_copies = exchange(lambda dst: st_stage, st_recv, ss_sem, sr_sem)
    st_recv[me] = st_stage[...]

    for s in range(slots):
        v_copies[s].wait()
        for k in range(KVH):
            expo, total = weights[s, k]
            part = jnp.dot(
                expo, v_vm[s, :, k * HEAD : (k + 1) * HEAD], preferred_element_type=jnp.float32
            )
            o_rows[pl.ds(k * group * slots + s, group, stride=slots), :] = part / total
    o_stage[...] = o_rows[...].reshape(n, heads_dev * slots, HEAD).astype(jnp.bfloat16)
    o_copies = exchange(lambda dst: o_stage.at[dst], o_recv, os_sem, or_sem)
    o_recv[me] = o_stage[me]

    for copy in st_copies:
        copy.wait_recv()
    every = st_recv[...].reshape(total_slots, 128)
    slot_top = jnp.zeros((total_slots, 128), jnp.float32)
    req_tops = []
    for r in range(requests):
        mine = slot_req == r + 1.0
        req_top = jnp.max(jnp.where(mine, every, floor_value), axis=0, keepdims=True)
        slot_top = jnp.where(mine, req_top, slot_top)
        req_tops.append(req_top)
    share = jnp.exp(every - slot_top)
    totals = dot_f32(belongs, share, ((1,), (0,)))
    log_norm = jnp.concatenate(req_tops, axis=0) + jnp.log(totals)
    norm_ref[...] = log_norm[:, :QH]
    e_rows[...] = jnp.transpose(share)

    for copy in o_copies:
        copy.wait_recv()
    parts = o_recv[...].astype(jnp.float32)
    for h in range(heads_dev):
        mix = belongs * e_rows[pl.ds(me * heads_dev + h, 1), :]
        value = dot_f32(
            mix,
            parts[:, h * slots : (h + 1) * slots, :].reshape(total_slots, HEAD),
            ((1,), (0,)),
        )
        value = value / jnp.sum(mix, axis=1, keepdims=True)
        out_ref[:, h * HEAD : (h + 1) * HEAD] = value.astype(jnp.bfloat16)

    for copy in q_copies + st_copies + o_copies:
        copy.wait_send()


def fused_body(n, queries, key_pages, value_pages, page_table, lengths):
    slots, page_rows, width = key_pages.shape
    requests = queries.shape[0]
    heads_dev = queries.shape[1] // HEAD
    vmem = pl.BlockSpec(memory_space=pltpu.VMEM)
    hbm = pl.BlockSpec(memory_space=pl.ANY)
    smem = pl.BlockSpec(memory_space=pltpu.SMEM)
    exchanged = (n, heads_dev * slots, HEAD)
    return pl.pallas_call(
        functools.partial(kernel, n),
        out_shape=(
            jax.ShapeDtypeStruct(queries.shape, jnp.bfloat16),
            jax.ShapeDtypeStruct((requests, QH), jnp.float32),
        ),
        in_specs=[vmem, hbm, hbm, vmem, smem],
        out_specs=(vmem, vmem),
        scratch_shapes=[
            pltpu.VMEM((slots, page_rows, width), jnp.bfloat16),
            pltpu.VMEM((slots, page_rows, width), jnp.bfloat16),
            pltpu.VMEM(exchanged, jnp.bfloat16),
            pltpu.VMEM(exchanged, jnp.bfloat16),
            pltpu.VMEM((QH * slots, HEAD), jnp.float32),
            pltpu.VMEM((QH * slots, HEAD), jnp.float32),
            pltpu.VMEM(exchanged, jnp.bfloat16),
            pltpu.VMEM(exchanged, jnp.bfloat16),
            pltpu.VMEM((slots, 128), jnp.float32),
            pltpu.VMEM((n, slots, 128), jnp.float32),
            pltpu.VMEM((128, n * slots), jnp.float32),
            pltpu.SemaphoreType.DMA((slots,)),
            pltpu.SemaphoreType.DMA((slots,)),
        ]
        + [pltpu.SemaphoreType.DMA((n,))] * 6,
        compiler_params=pltpu.CompilerParams(collective_id=0, has_side_effects=True),
    )(queries, key_pages, value_pages, page_table, lengths)


def body(queries, key_pages, value_pages, page_table, lengths):
    n = lax.axis_size("seq")
    slots, page_rows, _ = key_pages.shape
    whole_heads = queries.shape[1] % HEAD == 0
    whole_tiles = slots % 8 == 0 and (n * slots) % 128 == 0 and page_rows % 128 == 0
    if whole_heads and whole_tiles and slots <= 128:
        return fused_body(n, queries, key_pages, value_pages, page_table, lengths)
    return generic_body(queries, key_pages, value_pages, page_table, lengths)


def solution(mesh):
    placed = (
        P("rep", "seq"),
        P(("rep", "seq"), None, None),
        P(("rep", "seq"), None, None),
        P("rep", None),
        P("rep"),
    )
    return jax.shard_map(
        body,
        mesh=mesh,
        in_specs=placed,
        out_specs=(P("rep", "seq"), P("rep", None)),
        check_vma=False,
    )
```

```python
import functools
import math

import jax
import jax.numpy as jnp
from jax import lax
from jax.experimental import pallas as pl
from jax.experimental.pallas import tpu as pltpu
from jax.sharding import PartitionSpec as P

QH = 64
KVH = 8
HEAD = 128


floor_value = -1000000000.0


def attend_block(block_index, running, pool_keys, pool_values, pool_req, pool_tok, whole_queries):
    run_max, run_sum, run_out = running
    per_step = 4
    requests = whole_queries.shape[0]
    page_rows = pool_keys.shape[1]
    group_size = QH // KVH
    start_slot = block_index * per_step
    block_keys = lax.dynamic_slice_in_dim(pool_keys, start_slot, per_step, 0).reshape(
        per_step, page_rows, KVH, HEAD
    )
    block_values = lax.dynamic_slice_in_dim(pool_values, start_slot, per_step, 0).reshape(
        per_step, page_rows, KVH, HEAD
    )
    block_req = lax.dynamic_slice_in_dim(pool_req, start_slot, per_step, 0)
    block_tok = lax.dynamic_slice_in_dim(pool_tok, start_slot, per_step, 0)
    block_queries = whole_queries[block_req].reshape(per_step, KVH, group_size, HEAD)
    scores = jnp.einsum(
        "bkgd,btkd->bkgt", block_queries, block_keys, preferred_element_type=jnp.float32
    ) * (1.0 / math.sqrt(HEAD))
    is_valid = jnp.arange(page_rows, dtype=jnp.int32)[None, :] < block_tok[:, None]
    scores = jnp.where(is_valid[:, None, None, :], scores, floor_value)
    page_max = jnp.max(scores, axis=-1)
    weights = jnp.where(is_valid[:, None, None, :], jnp.exp(scores - page_max[..., None]), 0.0)
    page_sum = jnp.sum(weights, axis=-1).reshape(per_step, QH)
    page_out = jnp.einsum(
        "bkgt,btkd->bkgd",
        weights.astype(jnp.bfloat16),
        block_values,
        preferred_element_type=jnp.float32,
    ).reshape(per_step, QH, HEAD)
    page_max = page_max.reshape(per_step, QH)
    belongs = (block_req[:, None] == jnp.arange(requests, dtype=jnp.int32)[None, :]) & (
        block_tok[:, None] > 0
    )
    candidate = jnp.where(belongs[:, :, None], page_max[:, None, :], floor_value)
    new_max = jnp.maximum(run_max, jnp.max(candidate, axis=0))
    keep_scale = jnp.where(run_max > 0.5 * floor_value, jnp.exp(run_max - new_max), 0.0)
    mixing = jnp.where(belongs[:, :, None], jnp.exp(candidate - new_max[None, :, :]), 0.0)
    run_sum = run_sum * keep_scale + jnp.sum(mixing * page_sum[:, None, :], axis=0)
    run_out = run_out * keep_scale[:, :, None] + jnp.einsum(
        "brh,bhd->rhd", mixing, page_out, precision=lax.Precision.HIGHEST
    )
    return (run_max * 0.0 + new_max, run_sum, run_out)


def generic_body(queries, key_pages, value_pages, page_table, lengths):
    slot_count = key_pages.shape[0]
    page_rows = key_pages.shape[1]
    requests, max_pages = page_table.shape
    devices = lax.axis_size("seq")
    my_index = lax.axis_index("seq")
    whole_queries = lax.all_gather(queries, "seq", axis=1, tiled=True)
    entry_ids = page_table.reshape(-1)
    entry_req = jnp.repeat(jnp.arange(requests, dtype=jnp.int32), max_pages)
    entry_tok = jnp.clip(
        lengths[:, None] - jnp.arange(max_pages, dtype=jnp.int32)[None, :] * page_rows, 0, page_rows
    ).reshape(-1)
    entry_dev = jnp.where(entry_ids >= 0, entry_ids // slot_count, -1)
    local_ids = entry_ids - my_index * slot_count
    slot_range = jnp.arange(slot_count, dtype=jnp.int32)
    matches = (entry_dev[None, :] == my_index) & (local_ids[None, :] == slot_range[:, None])
    pool_req = jnp.sum(jnp.where(matches, entry_req[None, :], 0), axis=1)
    pool_tok = jnp.sum(jnp.where(matches, entry_tok[None, :], 0), axis=1)
    per_step = 4
    block_total = slot_count // per_step
    start_state = (
        jnp.full((requests, QH), floor_value, jnp.float32),
        jnp.zeros((requests, QH), jnp.float32),
        jnp.zeros((requests, QH, HEAD), jnp.float32),
    )

    def step_block(block_index, running):
        return attend_block(
            block_index, running, key_pages, value_pages, pool_req, pool_tok, whole_queries
        )

    run_max, run_sum, run_out = lax.fori_loop(0, block_total, step_block, start_state)
    width_dev = QH * HEAD // devices
    col_heads = (my_index * width_dev + jnp.arange(width_dev, dtype=jnp.int32)) // HEAD
    pieces = lax.all_to_all(
        run_out.reshape(requests, QH * HEAD).astype(jnp.bfloat16),
        "seq",
        split_axis=1,
        concat_axis=0,
        tiled=True,
    ).astype(jnp.float32)
    every_max, every_sum = (
        lax.all_gather(run_max[None], "seq", axis=0, tiled=True),
        lax.all_gather(run_sum[None], "seq", axis=0, tiled=True),
    )
    top_max = jnp.max(every_max, axis=0)
    factor = jnp.exp(every_max - top_max[None])
    totals = jnp.sum(every_sum * factor, axis=0)
    col_factor = jnp.take(factor, col_heads, axis=2)
    shares = jnp.sum(pieces.reshape(devices, requests, width_dev) * col_factor, axis=0)
    denominators = jnp.take(totals, col_heads, axis=1)
    attention_out = (shares / denominators).astype(jnp.bfloat16)
    log_norm = top_max + jnp.log(totals)
    return (attention_out, log_norm)


def dot_f32(a, b, contract):
    return lax.dot_general(
        a, b, (contract, ((), ())), precision=lax.Precision.HIGHEST, preferred_element_type=jnp.float32
    )


def kernel(
    n,
    q_ref,
    k_hbm,
    v_hbm,
    pt_ref,
    len_ref,
    out_ref,
    norm_ref,
    k_vm,
    v_vm,
    q_stage,
    q_recv,
    q_rows,
    o_rows,
    o_stage,
    o_recv,
    st_stage,
    st_recv,
    e_rows,
    k_sem,
    v_sem,
    qs_sem,
    qr_sem,
    os_sem,
    or_sem,
    ss_sem,
    sr_sem,
):
    me = lax.axis_index("seq")
    slots, page_rows = k_vm.shape[:2]
    max_pages, requests = pt_ref.shape
    total_slots = n * slots
    heads_dev = q_ref.shape[1] // HEAD
    group = QH // KVH

    k_copies = [pltpu.make_async_copy(k_hbm.at[s], k_vm.at[s], k_sem.at[s]) for s in range(slots)]
    v_copies = [pltpu.make_async_copy(v_hbm.at[s], v_vm.at[s], v_sem.at[s]) for s in range(slots)]
    for copy in k_copies + v_copies:
        copy.start()

    barrier = pltpu.get_barrier_semaphore()
    for i in range(1, n):
        pl.semaphore_signal(
            barrier, inc=1, device_id={"seq": lax.rem(me + i, n)}, device_id_type=pl.DeviceIdType.MESH
        )

    table = jnp.transpose(pt_ref[...])
    row_at = lax.broadcasted_iota(jnp.int32, (requests, 1), 0)
    len_col = jnp.zeros((requests, 1), jnp.int32)
    for r in range(requests):
        len_col = jnp.where(row_at == r, len_ref[r], len_col)
    slot_lane = lax.broadcasted_iota(jnp.int32, (requests, total_slots), 1)
    local_lane = lax.broadcasted_iota(jnp.int32, (requests, 128), 1)
    belongs = jnp.zeros((requests, total_slots), jnp.float32)
    local_tok = jnp.zeros((requests, 128), jnp.int32)
    for j in range(max_pages):
        entry = table[:, j : j + 1]
        belongs = jnp.where(slot_lane == entry, 1.0, belongs)
        tok = jnp.clip(len_col - j * page_rows, 0, page_rows)
        local_tok = jnp.where(local_lane + me * slots == entry, tok, local_tok)
    local_tok = jnp.max(local_tok, axis=0, keepdims=True)

    belongs_t = jnp.transpose(belongs)
    picked = jnp.dot(
        belongs_t.astype(jnp.bfloat16), q_ref[...], preferred_element_type=jnp.float32
    )
    picked = jnp.concatenate(
        [
            picked[:, h * HEAD : (h + 1) * HEAD].reshape(n, slots, HEAD)
            for h in range(heads_dev)
        ],
        axis=1,
    )
    q_stage[...] = picked.astype(jnp.bfloat16)
    req_col = lax.broadcasted_iota(jnp.int32, (requests, 128), 0).astype(jnp.bfloat16) + 1
    slot_req = jnp.dot(
        belongs_t.astype(jnp.bfloat16), req_col, preferred_element_type=jnp.float32
    )

    pl.semaphore_wait(barrier, n - 1)

    def exchange(stage_of, recv, send_sem, recv_sem):
        copies = []
        for i in range(1, n):
            dst = lax.rem(me + i, n)
            copies.append(
                pltpu.make_async_remote_copy(
                    src_ref=stage_of(dst),
                    dst_ref=recv.at[me],
                    send_sem=send_sem.at[i],
                    recv_sem=recv_sem.at[i],
                    device_id={"seq": dst},
                    device_id_type=pl.DeviceIdType.MESH,
                )
            )
            copies[-1].start()
        return copies

    q_copies = exchange(lambda dst: q_stage.at[dst], q_recv, qs_sem, qr_sem)
    q_recv[me] = q_stage[me]
    for copy in q_copies:
        copy.wait_recv()
    q_rows[...] = q_recv[...].astype(jnp.float32).reshape(QH * slots, HEAD)

    scale = 1.0 / math.sqrt(HEAD)
    tok_lane = lax.broadcasted_iota(jnp.int32, (group, page_rows), 1)
    stat_lane = lax.broadcasted_iota(jnp.int32, (group, 128), 1)
    tops = [jnp.zeros((group, 128), jnp.float32) for _ in range(KVH)]
    sums = [jnp.ones((group, 128), jnp.float32) for _ in range(KVH)]
    weights = {}
    for s in range(slots):
        k_copies[s].wait()
        is_valid = tok_lane < local_tok[:, s : s + 1]
        for k in range(KVH):
            q = q_rows[pl.ds(k * group * slots + s, group, stride=slots), :].astype(jnp.bfloat16)
            scores = lax.dot_general(
                q,
                k_vm[s, :, k * HEAD : (k + 1) * HEAD],
                (((1,), (1,)), ((), ())),
                preferred_element_type=jnp.float32,
            )
            scores = jnp.where(is_valid, scores * scale, floor_value)
            top = jnp.max(scores, axis=1, keepdims=True)
            expo = jnp.exp(scores - top)
            total = jnp.sum(expo, axis=1, keepdims=True)
            tops[k] = jnp.where(stat_lane == s, top, tops[k])
            sums[k] = jnp.where(stat_lane == s, total, sums[k])
            weights[s, k] = (expo.astype(jnp.bfloat16), total)
    lse = jnp.concatenate(tops, axis=0) + jnp.log(jnp.concatenate(sums, axis=0))
    lse = jnp.concatenate([lse, jnp.zeros((128 - QH, 128), jnp.float32)], axis=0)
    st_stage[...] = jnp.transpose(lse)[:slots]
    st_copies = exchange(lambda dst: st_stage, st_recv, ss_sem, sr_sem)
    st_recv[me] = st_stage[...]

    for s in range(slots):
        v_copies[s].wait()
        for k in range(KVH):
            expo, total = weights[s, k]
            part = jnp.dot(
                expo, v_vm[s, :, k * HEAD : (k + 1) * HEAD], preferred_element_type=jnp.float32
            )
            o_rows[pl.ds(k * group * slots + s, group, stride=slots), :] = part / total
    o_stage[...] = o_rows[...].reshape(n, heads_dev * slots, HEAD).astype(jnp.bfloat16)
    o_copies = exchange(lambda dst: o_stage.at[dst], o_recv, os_sem, or_sem)
    o_recv[me] = o_stage[me]

    for copy in st_copies:
        copy.wait_recv()
    every = st_recv[...].reshape(total_slots, 128)
    slot_top = jnp.zeros((total_slots, 128), jnp.float32)
    req_tops = []
    for r in range(requests):
        mine = slot_req == r + 1.0
        req_top = jnp.max(jnp.where(mine, every, floor_value), axis=0, keepdims=True)
        slot_top = jnp.where(mine, req_top, slot_top)
        req_tops.append(req_top)
    share = jnp.exp(every - slot_top)
    totals = dot_f32(belongs, share, ((1,), (0,)))
    log_norm = jnp.concatenate(req_tops, axis=0) + jnp.log(totals)
    norm_ref[...] = log_norm[:, :QH]
    e_rows[...] = jnp.transpose(share)

    for copy in o_copies:
        copy.wait_recv()
    parts = o_recv[...].astype(jnp.float32)
    for h in range(heads_dev):
        mix = belongs * e_rows[pl.ds(me * heads_dev + h, 1), :]
        value = dot_f32(
            mix,
            parts[:, h * slots : (h + 1) * slots, :].reshape(total_slots, HEAD),
            ((1,), (0,)),
        )
        value = value / jnp.sum(mix, axis=1, keepdims=True)
        out_ref[:, h * HEAD : (h + 1) * HEAD] = value.astype(jnp.bfloat16)

    for copy in q_copies + st_copies + o_copies:
        copy.wait_send()


def place(out_in, norm_in, out_ref, norm_ref):
    out_ref[...] = out_in[...]
    norm_ref[...] = norm_in[...]


def fused_body(n, queries, key_pages, value_pages, page_table, lengths):
    slots, page_rows, width = key_pages.shape
    requests = queries.shape[0]
    heads_dev = queries.shape[1] // HEAD
    vmem = pl.BlockSpec(memory_space=pltpu.VMEM)
    hbm = pl.BlockSpec(memory_space=pl.ANY)
    smem = pl.BlockSpec(memory_space=pltpu.SMEM)
    exchanged = (n, heads_dev * slots, HEAD)
    parts = pl.pallas_call(
        functools.partial(kernel, n),
        out_shape=(
            jax.ShapeDtypeStruct(queries.shape, jnp.bfloat16),
            jax.ShapeDtypeStruct((requests, QH), jnp.float32),
        ),
        in_specs=[vmem, hbm, hbm, vmem, smem],
        out_specs=(vmem, vmem),
        scratch_shapes=[
            pltpu.VMEM((slots, page_rows, width), jnp.bfloat16),
            pltpu.VMEM((slots, page_rows, width), jnp.bfloat16),
            pltpu.VMEM(exchanged, jnp.bfloat16),
            pltpu.VMEM(exchanged, jnp.bfloat16),
            pltpu.VMEM((QH * slots, HEAD), jnp.float32),
            pltpu.VMEM((QH * slots, HEAD), jnp.float32),
            pltpu.VMEM(exchanged, jnp.bfloat16),
            pltpu.VMEM(exchanged, jnp.bfloat16),
            pltpu.VMEM((slots, 128), jnp.float32),
            pltpu.VMEM((n, slots, 128), jnp.float32),
            pltpu.VMEM((128, n * slots), jnp.float32),
            pltpu.SemaphoreType.DMA((slots,)),
            pltpu.SemaphoreType.DMA((slots,)),
        ]
        + [pltpu.SemaphoreType.DMA((n,))] * 6,
        compiler_params=pltpu.CompilerParams(collective_id=0, has_side_effects=True),
    )(queries, key_pages, value_pages, page_table.T, lengths)
    return pl.pallas_call(
        place,
        out_shape=tuple(jax.ShapeDtypeStruct(a.shape, a.dtype) for a in parts),
        in_specs=[vmem] * 2,
        out_specs=(vmem, vmem),
    )(*parts)


def body(queries, key_pages, value_pages, page_table, lengths):
    n = lax.axis_size("seq")
    slots, page_rows, _ = key_pages.shape
    whole_heads = queries.shape[1] % HEAD == 0
    whole_tiles = slots % 8 == 0 and (n * slots) % 128 == 0 and page_rows % 128 == 0
    if whole_heads and whole_tiles and slots <= 128:
        return fused_body(n, queries, key_pages, value_pages, page_table, lengths)
    return generic_body(queries, key_pages, value_pages, page_table, lengths)


def solution(mesh):
    placed = (
        P("rep", "seq"),
        P(("rep", "seq"), None, None),
        P(("rep", "seq"), None, None),
        P("rep", None),
        P("rep"),
    )
    return jax.shard_map(
        body,
        mesh=mesh,
        in_specs=placed,
        out_specs=(P("rep", "seq"), P("rep", None)),
        check_vma=False,
    )
```

```python
import functools
import math

import jax
import jax.numpy as jnp
from jax import lax
from jax.experimental import pallas as pl
from jax.experimental.pallas import tpu as pltpu
from jax.sharding import PartitionSpec as P

QH = 64
KVH = 8
HEAD = 128


floor_value = -1000000000.0


def attend_block(block_index, running, pool_keys, pool_values, pool_req, pool_tok, whole_queries):
    run_max, run_sum, run_out = running
    per_step = 4
    requests = whole_queries.shape[0]
    page_rows = pool_keys.shape[1]
    group_size = QH // KVH
    start_slot = block_index * per_step
    block_keys = lax.dynamic_slice_in_dim(pool_keys, start_slot, per_step, 0).reshape(
        per_step, page_rows, KVH, HEAD
    )
    block_values = lax.dynamic_slice_in_dim(pool_values, start_slot, per_step, 0).reshape(
        per_step, page_rows, KVH, HEAD
    )
    block_req = lax.dynamic_slice_in_dim(pool_req, start_slot, per_step, 0)
    block_tok = lax.dynamic_slice_in_dim(pool_tok, start_slot, per_step, 0)
    block_queries = whole_queries[block_req].reshape(per_step, KVH, group_size, HEAD)
    scores = jnp.einsum(
        "bkgd,btkd->bkgt", block_queries, block_keys, preferred_element_type=jnp.float32
    ) * (1.0 / math.sqrt(HEAD))
    is_valid = jnp.arange(page_rows, dtype=jnp.int32)[None, :] < block_tok[:, None]
    scores = jnp.where(is_valid[:, None, None, :], scores, floor_value)
    page_max = jnp.max(scores, axis=-1)
    weights = jnp.where(is_valid[:, None, None, :], jnp.exp(scores - page_max[..., None]), 0.0)
    page_sum = jnp.sum(weights, axis=-1).reshape(per_step, QH)
    page_out = jnp.einsum(
        "bkgt,btkd->bkgd",
        weights.astype(jnp.bfloat16),
        block_values,
        preferred_element_type=jnp.float32,
    ).reshape(per_step, QH, HEAD)
    page_max = page_max.reshape(per_step, QH)
    belongs = (block_req[:, None] == jnp.arange(requests, dtype=jnp.int32)[None, :]) & (
        block_tok[:, None] > 0
    )
    candidate = jnp.where(belongs[:, :, None], page_max[:, None, :], floor_value)
    new_max = jnp.maximum(run_max, jnp.max(candidate, axis=0))
    keep_scale = jnp.where(run_max > 0.5 * floor_value, jnp.exp(run_max - new_max), 0.0)
    mixing = jnp.where(belongs[:, :, None], jnp.exp(candidate - new_max[None, :, :]), 0.0)
    run_sum = run_sum * keep_scale + jnp.sum(mixing * page_sum[:, None, :], axis=0)
    run_out = run_out * keep_scale[:, :, None] + jnp.einsum(
        "brh,bhd->rhd", mixing, page_out, precision=lax.Precision.HIGHEST
    )
    return (run_max * 0.0 + new_max, run_sum, run_out)


def generic_body(queries, key_pages, value_pages, page_table, lengths):
    slot_count = key_pages.shape[0]
    page_rows = key_pages.shape[1]
    requests, max_pages = page_table.shape
    devices = lax.axis_size("seq")
    my_index = lax.axis_index("seq")
    whole_queries = lax.all_gather(queries, "seq", axis=1, tiled=True)
    entry_ids = page_table.reshape(-1)
    entry_req = jnp.repeat(jnp.arange(requests, dtype=jnp.int32), max_pages)
    entry_tok = jnp.clip(
        lengths[:, None] - jnp.arange(max_pages, dtype=jnp.int32)[None, :] * page_rows, 0, page_rows
    ).reshape(-1)
    entry_dev = jnp.where(entry_ids >= 0, entry_ids // slot_count, -1)
    local_ids = entry_ids - my_index * slot_count
    slot_range = jnp.arange(slot_count, dtype=jnp.int32)
    matches = (entry_dev[None, :] == my_index) & (local_ids[None, :] == slot_range[:, None])
    pool_req = jnp.sum(jnp.where(matches, entry_req[None, :], 0), axis=1)
    pool_tok = jnp.sum(jnp.where(matches, entry_tok[None, :], 0), axis=1)
    per_step = 4
    block_total = slot_count // per_step
    start_state = (
        jnp.full((requests, QH), floor_value, jnp.float32),
        jnp.zeros((requests, QH), jnp.float32),
        jnp.zeros((requests, QH, HEAD), jnp.float32),
    )

    def step_block(block_index, running):
        return attend_block(
            block_index, running, key_pages, value_pages, pool_req, pool_tok, whole_queries
        )

    run_max, run_sum, run_out = lax.fori_loop(0, block_total, step_block, start_state)
    width_dev = QH * HEAD // devices
    col_heads = (my_index * width_dev + jnp.arange(width_dev, dtype=jnp.int32)) // HEAD
    pieces = lax.all_to_all(
        run_out.reshape(requests, QH * HEAD).astype(jnp.bfloat16),
        "seq",
        split_axis=1,
        concat_axis=0,
        tiled=True,
    ).astype(jnp.float32)
    every_max, every_sum = (
        lax.all_gather(run_max[None], "seq", axis=0, tiled=True),
        lax.all_gather(run_sum[None], "seq", axis=0, tiled=True),
    )
    top_max = jnp.max(every_max, axis=0)
    factor = jnp.exp(every_max - top_max[None])
    totals = jnp.sum(every_sum * factor, axis=0)
    col_factor = jnp.take(factor, col_heads, axis=2)
    shares = jnp.sum(pieces.reshape(devices, requests, width_dev) * col_factor, axis=0)
    denominators = jnp.take(totals, col_heads, axis=1)
    attention_out = (shares / denominators).astype(jnp.bfloat16)
    log_norm = top_max + jnp.log(totals)
    return (attention_out, log_norm)


def dot_f32(a, b, contract):
    return lax.dot_general(
        a, b, (contract, ((), ())), precision=lax.Precision.HIGHEST, preferred_element_type=jnp.float32
    )


def kernel(
    n,
    q_ref,
    k_hbm,
    v_hbm,
    pt_ref,
    len_ref,
    out_ref,
    norm_ref,
    k_vm,
    v_vm,
    q_stage,
    q_recv,
    q_rows,
    o_rows,
    o_stage,
    o_recv,
    st_stage,
    st_recv,
    e_rows,
    w_rows,
    t_rows,
    k_sem,
    v_sem,
    qs_sem,
    qr_sem,
    os_sem,
    or_sem,
    ss_sem,
    sr_sem,
):
    me = lax.axis_index("seq")
    slots, page_rows = k_vm.shape[:2]
    max_pages, requests = pt_ref.shape
    total_slots = n * slots
    heads_dev = q_ref.shape[1] // HEAD
    group = QH // KVH

    k_copies = [pltpu.make_async_copy(k_hbm.at[s], k_vm.at[s], k_sem.at[s]) for s in range(slots)]
    v_copies = [pltpu.make_async_copy(v_hbm.at[s], v_vm.at[s], v_sem.at[s]) for s in range(slots)]
    for copy in k_copies + v_copies:
        copy.start()

    barrier = pltpu.get_barrier_semaphore()
    for i in range(1, n):
        pl.semaphore_signal(
            barrier, inc=1, device_id={"seq": lax.rem(me + i, n)}, device_id_type=pl.DeviceIdType.MESH
        )

    table = jnp.transpose(pt_ref[...])
    row_at = lax.broadcasted_iota(jnp.int32, (requests, 1), 0)
    len_col = jnp.zeros((requests, 1), jnp.int32)
    for r in range(requests):
        len_col = jnp.where(row_at == r, len_ref[r], len_col)
    slot_lane = lax.broadcasted_iota(jnp.int32, (requests, total_slots), 1)
    local_lane = lax.broadcasted_iota(jnp.int32, (requests, 128), 1)
    belongs = jnp.zeros((requests, total_slots), jnp.float32)
    local_tok = jnp.zeros((requests, 128), jnp.int32)
    for j in range(max_pages):
        entry = table[:, j : j + 1]
        belongs = jnp.where(slot_lane == entry, 1.0, belongs)
        tok = jnp.clip(len_col - j * page_rows, 0, page_rows)
        local_tok = jnp.where(local_lane + me * slots == entry, tok, local_tok)
    local_tok = jnp.max(local_tok, axis=0, keepdims=True)

    belongs_t = jnp.transpose(belongs)
    picked = jnp.dot(
        belongs_t.astype(jnp.bfloat16), q_ref[...], preferred_element_type=jnp.float32
    )
    picked = jnp.concatenate(
        [
            picked[:, h * HEAD : (h + 1) * HEAD].reshape(n, slots, HEAD)
            for h in range(heads_dev)
        ],
        axis=1,
    )
    q_stage[...] = picked.astype(jnp.bfloat16)
    req_col = lax.broadcasted_iota(jnp.int32, (requests, 128), 0).astype(jnp.bfloat16) + 1
    slot_req = jnp.dot(
        belongs_t.astype(jnp.bfloat16), req_col, preferred_element_type=jnp.float32
    )

    pl.semaphore_wait(barrier, n - 1)

    def exchange(stage_of, recv, send_sem, recv_sem):
        copies = []
        for i in range(1, n):
            dst = lax.rem(me + i, n)
            copies.append(
                pltpu.make_async_remote_copy(
                    src_ref=stage_of(dst),
                    dst_ref=recv.at[me],
                    send_sem=send_sem.at[i],
                    recv_sem=recv_sem.at[i],
                    device_id={"seq": dst},
                    device_id_type=pl.DeviceIdType.MESH,
                )
            )
            copies[-1].start()
        return copies

    q_copies = exchange(lambda dst: q_stage.at[dst], q_recv, qs_sem, qr_sem)
    q_recv[me] = q_stage[me]
    for copy in q_copies:
        copy.wait_recv()
    q_rows[...] = q_recv[...].astype(jnp.float32).reshape(QH * slots, HEAD)

    scale = 1.0 / math.sqrt(HEAD)
    tok_lane = lax.broadcasted_iota(jnp.int32, (group, page_rows), 1)
    stat_lane = lax.broadcasted_iota(jnp.int32, (group, 128), 1)
    tops = [jnp.zeros((group, 128), jnp.float32) for _ in range(KVH)]
    sums = [jnp.ones((group, 128), jnp.float32) for _ in range(KVH)]
    for s in range(slots):
        k_copies[s].wait()
        is_valid = tok_lane < local_tok[:, s : s + 1]
        for k in range(KVH):
            q = q_rows[pl.ds(k * group * slots + s, group, stride=slots), :].astype(jnp.bfloat16)
            scores = lax.dot_general(
                q,
                k_vm[s, :, k * HEAD : (k + 1) * HEAD],
                (((1,), (1,)), ((), ())),
                preferred_element_type=jnp.float32,
            )
            scores = jnp.where(is_valid, scores * scale, floor_value)
            top = jnp.max(scores, axis=1, keepdims=True)
            expo = jnp.exp(scores - top)
            total = jnp.sum(expo, axis=1, keepdims=True)
            tops[k] = jnp.where(stat_lane == s, top, tops[k])
            sums[k] = jnp.where(stat_lane == s, total, sums[k])
            w_rows[k, s * group : (s + 1) * group, :] = expo
            t_rows[k, s * group : (s + 1) * group, :] = jnp.broadcast_to(1.0 / total, expo.shape)
    lse = jnp.concatenate(tops, axis=0) + jnp.log(jnp.concatenate(sums, axis=0))
    lse = jnp.concatenate([lse, jnp.zeros((128 - QH, 128), jnp.float32)], axis=0)
    st_stage[...] = jnp.transpose(lse)[:slots]
    st_copies = exchange(lambda dst: st_stage, st_recv, ss_sem, sr_sem)
    st_recv[me] = st_stage[...]

    for copy in v_copies:
        copy.wait()
    per = group // heads_dev
    my_core = lax.rem(me, per)
    middle = KVH // 2
    order = [middle]
    for away in range(middle - 1, 0, -1):
        order += [away, KVH - away]
    o_copies = []
    for step in order + [0]:
        k = lax.rem(me // per + step, KVH)
        column = pl.multiple_of(k * HEAD, HEAD)
        base = pl.multiple_of(k * group * slots, group * slots)
        for s in range(slots):
            rows = slice(s * group, (s + 1) * group)
            part = jnp.dot(
                w_rows[k, rows, :].astype(jnp.bfloat16),
                v_vm[s, :, pl.ds(column, HEAD)],
                preferred_element_type=jnp.float32,
            )
            o_rows[pl.ds(base + s, group, stride=slots), :] = part * t_rows[k, rows, :]
        done = o_rows[pl.ds(base, group * slots), :].astype(jnp.bfloat16)
        o_stage[pl.ds(k * per, per)] = done.reshape(per, heads_dev * slots, HEAD)
        for turn in range(per) if step else range(1, per):
            dst = k * per + lax.rem(my_core + turn, per)
            o_copies.append(
                pltpu.make_async_remote_copy(
                    src_ref=o_stage.at[dst],
                    dst_ref=o_recv.at[me],
                    send_sem=os_sem.at[step * per + turn],
                    recv_sem=or_sem.at[step * per + turn],
                    device_id={"seq": dst},
                    device_id_type=pl.DeviceIdType.MESH,
                )
            )
            o_copies[-1].start()
    o_recv[me] = o_stage[me]

    for copy in st_copies:
        copy.wait_recv()
    every = st_recv[...].reshape(total_slots, 128)
    slot_top = jnp.zeros((total_slots, 128), jnp.float32)
    req_tops = []
    for r in range(requests):
        mine = slot_req == r + 1.0
        req_top = jnp.max(jnp.where(mine, every, floor_value), axis=0, keepdims=True)
        slot_top = jnp.where(mine, req_top, slot_top)
        req_tops.append(req_top)
    share = jnp.exp(every - slot_top)
    totals = dot_f32(belongs, share, ((1,), (0,)))
    log_norm = jnp.concatenate(req_tops, axis=0) + jnp.log(totals)
    norm_ref[...] = log_norm[:, :QH]
    e_rows[...] = jnp.transpose(share)

    for copy in o_copies:
        copy.wait_recv()
    parts = o_recv[...].astype(jnp.float32)
    for h in range(heads_dev):
        mix = belongs * e_rows[pl.ds(me * heads_dev + h, 1), :]
        value = dot_f32(
            mix,
            parts[:, h * slots : (h + 1) * slots, :].reshape(total_slots, HEAD),
            ((1,), (0,)),
        )
        value = value / jnp.sum(mix, axis=1, keepdims=True)
        out_ref[:, h * HEAD : (h + 1) * HEAD] = value.astype(jnp.bfloat16)

    for copy in q_copies + st_copies + o_copies:
        copy.wait_send()


def place(out_in, norm_in, out_ref, norm_ref):
    out_ref[...] = out_in[...]
    norm_ref[...] = norm_in[...]


def fused_body(n, queries, key_pages, value_pages, page_table, lengths):
    slots, page_rows, width = key_pages.shape
    requests = queries.shape[0]
    heads_dev = queries.shape[1] // HEAD
    vmem = pl.BlockSpec(memory_space=pltpu.VMEM)
    hbm = pl.BlockSpec(memory_space=pl.ANY)
    smem = pl.BlockSpec(memory_space=pltpu.SMEM)
    exchanged = (n, heads_dev * slots, HEAD)
    parts = pl.pallas_call(
        functools.partial(kernel, n),
        out_shape=(
            jax.ShapeDtypeStruct(queries.shape, jnp.bfloat16),
            jax.ShapeDtypeStruct((requests, QH), jnp.float32),
        ),
        in_specs=[vmem, hbm, hbm, vmem, smem],
        out_specs=(vmem, vmem),
        scratch_shapes=[
            pltpu.VMEM((slots, page_rows, width), jnp.bfloat16),
            pltpu.VMEM((slots, page_rows, width), jnp.bfloat16),
            pltpu.VMEM(exchanged, jnp.bfloat16),
            pltpu.VMEM(exchanged, jnp.bfloat16),
            pltpu.VMEM((QH * slots, HEAD), jnp.float32),
            pltpu.VMEM((QH * slots, HEAD), jnp.float32),
            pltpu.VMEM(exchanged, jnp.bfloat16),
            pltpu.VMEM(exchanged, jnp.bfloat16),
            pltpu.VMEM((slots, 128), jnp.float32),
            pltpu.VMEM((n, slots, 128), jnp.float32),
            pltpu.VMEM((128, n * slots), jnp.float32),
            pltpu.VMEM((KVH, QH // KVH * slots, page_rows), jnp.float32),
            pltpu.VMEM((KVH, QH // KVH * slots, page_rows), jnp.float32),
            pltpu.SemaphoreType.DMA((slots,)),
            pltpu.SemaphoreType.DMA((slots,)),
        ]
        + [pltpu.SemaphoreType.DMA((n,))] * 6,
        compiler_params=pltpu.CompilerParams(collective_id=0, has_side_effects=True),
    )(queries, key_pages, value_pages, page_table.T, lengths)
    return pl.pallas_call(
        place,
        out_shape=tuple(jax.ShapeDtypeStruct(a.shape, a.dtype) for a in parts),
        in_specs=[vmem] * 2,
        out_specs=(vmem, vmem),
    )(*parts)


def body(queries, key_pages, value_pages, page_table, lengths):
    n = lax.axis_size("seq")
    slots, page_rows, _ = key_pages.shape
    whole_heads = queries.shape[1] % HEAD == 0
    whole_tiles = slots % 8 == 0 and (n * slots) % 128 == 0 and page_rows % 128 == 0
    whole_tiles = whole_tiles and page_rows == HEAD
    if whole_heads and whole_tiles and slots <= 128 and n % KVH == 0:
        return fused_body(n, queries, key_pages, value_pages, page_table, lengths)
    return generic_body(queries, key_pages, value_pages, page_table, lengths)


def solution(mesh):
    placed = (
        P("rep", "seq"),
        P(("rep", "seq"), None, None),
        P(("rep", "seq"), None, None),
        P("rep", None),
        P("rep"),
    )
    return jax.shard_map(
        body,
        mesh=mesh,
        in_specs=placed,
        out_specs=(P("rep", "seq"), P("rep", None)),
        check_vma=False,
    )
```
